8 devices in a mesh: tp: 2 (over z, y), dp: 4 (over x, core).
Axes of the slice: x: 2, y: 2, z: 1, core: 2. Of those that a mesh axis runs over, the one named last changes fastest.
Arguments:
- prompts: bfloat16 [16, 1024, 4096], P('dp')
- lengths: int32 [16], P('dp')
- targets: int32 [16], P('dp')
- norm_attn: bfloat16 [1, 4096], replicated
- norm_mlp: bfloat16 [1, 4096], replicated
- norm_final: bfloat16 [4096], replicated
- w_query: bfloat16 [1, 4096, 4096], P(None, ('dp', 'tp'))
- w_key: bfloat16 [1, 4096, 1024], P(None, ('dp', 'tp'))
- w_value: bfloat16 [1, 4096, 1024], P(None, ('dp', 'tp'))
- w_out: bfloat16 [1, 4096, 4096], P(None, ('dp', 'tp'))
- w_gate: bfloat16 [1, 4096, 14336], P(None, ('dp', 'tp'))
- w_up: bfloat16 [1, 4096, 14336], P(None, ('dp', 'tp'))
- w_down: bfloat16 [1, 14336, 4096], P(None, ('dp', 'tp'))
- w_head: bfloat16 [4096, 32000], P(('dp', 'tp'))
Outputs:
- output 1: bfloat16 [1, 4096, 4096], P(None, None, 'tp')
- output 2: bfloat16 [1, 4096, 1024], P(None, None, 'tp')
- output 3: bfloat16 [1, 4096, 1024], P(None, None, 'tp')
- output 4: bfloat16 [1, 4096, 4096], P(None, 'tp')
- output 5: bfloat16 [1, 4096, 14336], P(None, None, 'tp')
- output 6: bfloat16 [1, 4096, 14336], P(None, None, 'tp')
- output 7: bfloat16 [1, 14336, 4096], P(None, 'tp')
- output 8: bfloat16 [4096, 32000], P(None, 'tp')
- output 9: bfloat16 [1, 16, 8, 1024, 128], P(None, 'dp', 'tp')
- output 10: bfloat16 [1, 16, 8, 1024, 128], P(None, 'dp', 'tp')
- output 11: float32 [16], P('dp')
All inputs are finite; a program needn't handle non-finite values.
Results may differ from the reference program's by a relative error of at most 0.00231272.
Values are sent between devices in bfloat16 or wider.
A program may use at most 2 GiB of HBM per device.

```python
import jax
import jax.numpy as jnp
from jax import lax

MODEL_DIM = 4096
NUM_HEADS = 32
KV_HEADS = 8
HEAD_DIM = 128
FFN_DIM = 14336
VOCAB_SIZE = 32000
LAYERS = 1
SEQ_LEN = 1024
BATCH_ALL = 16
TP_SIZE = 2
RMS_EPS = 1e-5
ROPE_BASE = 10000.0
GROUP_SIZE = NUM_HEADS // KV_HEADS


def setup_inputs(seed: int = 0) -> dict:
    key_list = jax.random.split(jax.random.key(seed), 14)

    def draw_normal(key_one, arr_shape, std_scale):
        return (jax.random.normal(key_one, arr_shape, jnp.float32) * std_scale).astype(jnp.bfloat16)

    def draw_gains(key_one, arr_shape):
        return (1.0 + 0.3 * jax.random.normal(key_one, arr_shape, jnp.float32)).astype(jnp.bfloat16)

    q_width = NUM_HEADS * HEAD_DIM
    kv_width = KV_HEADS * HEAD_DIM
    lengths = jax.random.randint(key_list[1], (BATCH_ALL,), 1, SEQ_LEN + 1, jnp.int32).at[0].set(SEQ_LEN)
    targets = jax.random.randint(key_list[2], (BATCH_ALL,), 0, VOCAB_SIZE, jnp.int32)
    return {
        "prompts": draw_normal(key_list[0], (BATCH_ALL, SEQ_LEN, MODEL_DIM), 1.0),
        "lengths": lengths,
        "targets": targets,
        "norm_attn": draw_gains(key_list[3], (LAYERS, MODEL_DIM)),
        "norm_mlp": draw_gains(key_list[4], (LAYERS, MODEL_DIM)),
        "norm_final": draw_gains(key_list[5], (MODEL_DIM,)),
        "w_query": draw_normal(key_list[6], (LAYERS, MODEL_DIM, q_width), MODEL_DIM ** -0.5),
        "w_key": draw_normal(key_list[7], (LAYERS, MODEL_DIM, kv_width), MODEL_DIM ** -0.5),
        "w_value": draw_normal(key_list[8], (LAYERS, MODEL_DIM, kv_width), MODEL_DIM ** -0.5),
        "w_out": draw_normal(key_list[9], (LAYERS, q_width, MODEL_DIM), q_width ** -0.5),
        "w_gate": draw_normal(key_list[10], (LAYERS, MODEL_DIM, FFN_DIM), MODEL_DIM ** -0.5),
        "w_up": draw_normal(key_list[11], (LAYERS, MODEL_DIM, FFN_DIM), MODEL_DIM ** -0.5),
        "w_down": draw_normal(key_list[12], (LAYERS, FFN_DIM, MODEL_DIM), FFN_DIM ** -0.5),
        "w_head": draw_normal(key_list[13], (MODEL_DIM, VOCAB_SIZE), 2.0 * MODEL_DIM ** -0.5),
    }


def rms_norm(hidden, gain):
    hidden_f32 = hidden.astype(jnp.float32)
    inv_rms = lax.rsqrt(jnp.mean(hidden_f32 * hidden_f32, axis=-1, keepdims=True) + RMS_EPS)
    return (hidden_f32 * inv_rms * gain.astype(jnp.float32)).astype(jnp.bfloat16)


def rotate(projected, cosines, sines):
    half_dim = HEAD_DIM // 2
    first_half = projected[..., :half_dim]
    second_half = projected[..., half_dim:]
    return jnp.concatenate([first_half * cosines - second_half * sines, second_half * cosines + first_half * sines], axis=-1)


def split_sum(acts, weight):
    inner_dim = acts.shape[-1]
    acts_split = acts.reshape(SEQ_LEN, TP_SIZE, inner_dim // TP_SIZE).astype(jnp.float32)
    weight_split = weight.reshape(TP_SIZE, inner_dim // TP_SIZE, MODEL_DIM).astype(jnp.float32)
    partials = jnp.einsum("spk,pkd->psd", acts_split, weight_split).astype(jnp.bfloat16)
    return jnp.sum(partials.astype(jnp.float32), axis=0)


def sequence_forward(tokens, length, target, norm_attn, norm_mlp, norm_final, w_query, w_key, w_value, w_out, w_gate, w_up, w_down, w_head):
    positions = jnp.arange(SEQ_LEN)
    inv_freq = ROPE_BASE ** (-jnp.arange(HEAD_DIM // 2, dtype=jnp.float32) * (2.0 / HEAD_DIM))
    angles = positions.astype(jnp.float32)[:, None, None] * inv_freq[None, None, :]
    cosines = jnp.cos(angles)
    sines = jnp.sin(angles)
    key_ok = (positions[None, :] <= positions[:, None]) & (positions[None, :] < length)

    def layer_step(hidden, params):
        gain_attn, gain_mlp, q_weight, k_weight, v_weight, o_weight, gate_weight, up_weight, down_weight = params
        normed = rms_norm(hidden, gain_attn)
        queries = jnp.dot(normed, q_weight, preferred_element_type=jnp.float32).reshape(SEQ_LEN, NUM_HEADS, HEAD_DIM)
        keys_raw = jnp.dot(normed, k_weight, preferred_element_type=jnp.float32).reshape(SEQ_LEN, KV_HEADS, HEAD_DIM)
        values = jnp.dot(normed, v_weight, preferred_element_type=jnp.float32).astype(jnp.bfloat16).reshape(SEQ_LEN, KV_HEADS, HEAD_DIM)
        queries = rotate(queries, cosines, sines).astype(jnp.bfloat16).reshape(SEQ_LEN, KV_HEADS, GROUP_SIZE, HEAD_DIM)
        keys_rot = rotate(keys_raw, cosines, sines).astype(jnp.bfloat16)
        scores = jnp.einsum("qkgh,skh->kgqs", queries.astype(jnp.float32), keys_rot.astype(jnp.float32)) * HEAD_DIM ** -0.5
        attn_probs = jax.nn.softmax(jnp.where(key_ok, scores, -1e30), axis=-1).astype(jnp.bfloat16)
        attn_out = jnp.einsum("kgqs,skh->qkgh", attn_probs.astype(jnp.float32), values.astype(jnp.float32))
        attn_out = attn_out.astype(jnp.bfloat16).reshape(SEQ_LEN, NUM_HEADS * HEAD_DIM)
        hidden = (hidden.astype(jnp.float32) + split_sum(attn_out, o_weight)).astype(jnp.bfloat16)
        normed_mlp = rms_norm(hidden, gain_mlp)
        gate_proj = jnp.dot(normed_mlp, gate_weight, preferred_element_type=jnp.float32)
        up_proj = jnp.dot(normed_mlp, up_weight, preferred_element_type=jnp.float32)
        mlp_act = (jax.nn.silu(gate_proj) * up_proj).astype(jnp.bfloat16)
        hidden = (hidden.astype(jnp.float32) + split_sum(mlp_act, down_weight)).astype(jnp.bfloat16)
        return hidden, (jnp.transpose(keys_rot, (1, 0, 2)), jnp.transpose(values, (1, 0, 2)))

    hidden, caches = lax.scan(layer_step, tokens, (norm_attn, norm_mlp, w_query, w_key, w_value, w_out, w_gate, w_up, w_down))
    last_row = lax.dynamic_index_in_dim(hidden, length - 1, axis=0, keepdims=False)
    logits = jnp.dot(rms_norm(last_row, norm_final), w_head, preferred_element_type=jnp.float32)
    picked = lax.dynamic_index_in_dim(logits, target, axis=0, keepdims=False)
    return caches[0], caches[1], picked - jax.nn.logsumexp(logits)


def reference(prompts, lengths, targets, norm_attn, norm_mlp, norm_final, w_query, w_key, w_value, w_out, w_gate, w_up, w_down, w_head):
    def per_sequence(seq_item):
        tokens, length, target = seq_item
        return sequence_forward(tokens, length, target, norm_attn, norm_mlp, norm_final, w_query, w_key, w_value, w_out, w_gate, w_up, w_down, w_head)

    key_all, value_all, logprobs = lax.map(per_sequence, (prompts, lengths, targets))
    return (w_query, w_key, w_value, w_out, w_gate, w_up, w_down, w_head, jnp.swapaxes(key_all, 0, 1), jnp.swapaxes(value_all, 0, 1), logprobs)
```

```python
import functools

import jax
import jax.numpy as jnp
from jax import lax
from jax.experimental import pallas as pl
from jax.experimental.pallas import tpu as pltpu
from jax.sharding import PartitionSpec as P


HEAD_DIM = 128
RMS_EPS = 1e-5
ROPE_BASE = 10000.0
SLOTS = 8
LAG = 4
TILE_BYTES = 1 << 20

HEAD_CUTS = (0, 256, 384, 448, 480, 512)
HEAD_TILE = 128
LOGIT_ROWS = 16


def rms_norm(hidden, gain):
    hidden_f32 = hidden.astype(jnp.float32)
    inv_rms = lax.rsqrt(jnp.mean(hidden_f32 * hidden_f32, axis=-1, keepdims=True) + RMS_EPS)
    return (hidden_f32 * inv_rms * gain.astype(jnp.float32)).astype(jnp.bfloat16)


def rotate(projected, cosines, sines):
    half_dim = HEAD_DIM // 2
    first_half = projected[..., :half_dim]
    second_half = projected[..., half_dim:]
    return jnp.concatenate([first_half * cosines - second_half * sines, second_half * cosines + first_half * sines], axis=-1)


def angles_at(positions):
    inv_freq = ROPE_BASE ** (-jnp.arange(HEAD_DIM // 2, dtype=jnp.float32) * (2.0 / HEAD_DIM))
    angles = positions.astype(jnp.float32)[..., None, None] * inv_freq
    return jnp.cos(angles), jnp.sin(angles)


def place_kernel(steps, n_in, n_alias, n_out, slot_of, *refs):
    ins = refs[:n_in]
    outs = refs[n_in + n_alias : n_in + n_alias + n_out]
    buf, in_sem, out_sem = refs[n_in + n_alias + n_out :]
    me = lax.axis_index("dp") * 2 + lax.axis_index("tp")

    def load(s):
        piece, row, rows, cols, _ = steps[s]
        slot = s % SLOTS
        return pltpu.make_async_copy(ins[piece].at[pl.ds(row, rows)], buf.at[slot, pl.ds(0, rows), pl.ds(0, cols)], in_sem.at[slot])

    def stores(s):
        piece, row, rows, _, dests = steps[s]
        slot = s % SLOTS
        for out, base, stride, first, width in dests:
            at = base + slot_of(piece, me) * stride + row
            yield pltpu.make_async_copy(
                buf.at[slot, pl.ds(0, rows), pl.ds(first, width)],
                outs[out].at[pl.ds(pl.multiple_of(at, 8), rows)],
                out_sem.at[slot],
            )

    total = len(steps)
    for s in range(total + LAG):
        if s < total:
            if s >= SLOTS:
                for copy in stores(s - SLOTS):
                    copy.wait()
            load(s).start()
        if s >= LAG:
            load(s - LAG).wait()
            for copy in stores(s - LAG):
                copy.start()
    for s in range(max(0, total - SLOTS), total):
        for copy in stores(s):
            copy.wait()


def place(pieces, outputs, slot_of, stride, base=0, into=None):
    rows, cols = pieces[0].shape
    tile = rows
    while tile * cols * 2 > TILE_BYTES and tile % 16 == 0:
        tile //= 2
    steps = []
    for piece in range(len(pieces)):
        for row in range(0, rows, tile):
            dests = [(out, base, stride, first, shape[1]) for out, (shape, first) in enumerate(outputs)]
            steps.append((piece, row, tile, cols, dests))
    alias = [] if into is None else list(into)
    return pl.pallas_call(
        functools.partial(place_kernel, steps, len(pieces), len(alias), len(outputs), slot_of),
        out_shape=[jax.ShapeDtypeStruct(shape, jnp.bfloat16) for shape, _ in outputs],
        in_specs=[pl.BlockSpec(memory_space=pl.ANY)] * (len(pieces) + len(alias)),
        out_specs=[pl.BlockSpec(memory_space=pl.ANY)] * len(outputs),
        scratch_shapes=[
            pltpu.VMEM((SLOTS, tile, cols), jnp.bfloat16),
            pltpu.SemaphoreType.DMA((SLOTS,)),
            pltpu.SemaphoreType.DMA((SLOTS,)),
        ],
        input_output_aliases={len(pieces) + k: k for k in range(len(alias))},
        compiler_params=pltpu.CompilerParams(vmem_limit_bytes=24 << 20),
    )(*pieces, *alias)


def head_kernel(rows, tile, n_in, n_alias, slot_of, *refs):
    z_ref, acc_ref = refs[:2]
    ins = refs[2 : 2 + n_in]
    out_ref, logits_ref, buf, in_sem, out_sem = refs[2 + n_in + n_alias :]
    me = lax.axis_index("dp") * 2 + lax.axis_index("tp")
    base, block, slots, lag = rows
    cols = out_ref.shape[1]
    steps = [(piece, row) for piece in range(n_in) for row in range(0, ins[0].shape[0], tile)]

    def load(s):
        piece, row = steps[s]
        slot = s % slots
        return pltpu.make_async_copy(ins[piece].at[pl.ds(row, tile)], buf.at[slot], in_sem.at[slot])

    def store(s):
        piece, row = steps[s]
        slot = s % slots
        at = pl.multiple_of(slot_of(piece, me) * block + base + row, 8)
        return pltpu.make_async_copy(buf.at[slot], out_ref.at[pl.ds(at, tile)], out_sem.at[slot])

    logits_ref[...] = acc_ref[...]
    width = cols // 5
    total = len(steps)
    for s in range(total + lag):
        if s < total:
            if s >= slots:
                store(s - slots).wait()
            load(s).start()
        if s >= lag:
            done = s - lag
            piece, row = steps[done]
            load(done).wait()
            store(done).start()
            z = z_ref[slot_of(piece, me)][:, row : row + tile]

            @pl.loop(0, 5)
            def _(j, z=z, slot=done % slots):
                at = pl.ds(pl.multiple_of(j * width, 128), width)
                logits_ref[:, at] += jnp.dot(z, buf[slot, :, at], preferred_element_type=jnp.float32)

    for s in range(max(0, total - slots), total):
        store(s).wait()


def place_head(pieces, shape, slot_of, block, base, z, acc, into):
    rows, cols = pieces[0].shape
    tile = min(rows, HEAD_TILE)
    slots, lag = 5, 2
    alias = [] if into is None else [into]
    any_spec = pl.BlockSpec(memory_space=pl.ANY)
    vmem = pl.BlockSpec(memory_space=pltpu.VMEM)
    return pl.pallas_call(
        functools.partial(head_kernel, (base, block, slots, lag), tile, len(pieces), len(alias), slot_of),
        out_shape=[jax.ShapeDtypeStruct(shape, jnp.bfloat16), jax.ShapeDtypeStruct(acc.shape, jnp.float32)],
        in_specs=[vmem, vmem] + [any_spec] * (len(pieces) + len(alias)),
        out_specs=[any_spec, vmem],
        scratch_shapes=[
            pltpu.VMEM((slots, tile, cols), jnp.bfloat16),
            pltpu.SemaphoreType.DMA((slots,)),
            pltpu.SemaphoreType.DMA((slots,)),
        ],
        input_output_aliases={2 + len(pieces): 0} if alias else {},
        compiler_params=pltpu.CompilerParams(vmem_limit_bytes=40 << 20),
    )(z, acc, *pieces, *alias)


def solution(mesh):
    tp_size = mesh.shape["tp"]
    dp_size = mesh.shape["dp"]
    train_spec = P(None, ("dp", "tp"), None)
    col_spec = P(None, None, "tp")
    row_spec = P(None, "tp", None)
    cache_spec = P(None, "dp", "tp", None, None)
    x_pairs = [(i, i ^ 2) for i in range(dp_size)]
    core_pairs = [(i, i ^ 1) for i in range(dp_size)]
    y_pairs = [(0, 1), (1, 0)]

    def over_x(value):
        return lax.ppermute(value, "dp", x_pairs)

    def over_y(value):
        return lax.ppermute(value, "tp", y_pairs)

    def over_core(value):
        return lax.ppermute(value, "dp", core_pairs)

    def layer_program(prompts, lengths, targets, norm_attn, norm_mlp, norm_final, w_query, w_key, w_value, w_out, w_gate, w_up, w_down, w_head):
        tp_idx = lax.axis_index("tp")
        dp_idx = lax.axis_index("dp")

        def halves(mats, rows=None):
            own, other = [], []
            for mat in mats:
                first, last = (0, mat.shape[0]) if rows is None else rows
                half = mat.shape[1] // 2
                own.append(lax.dynamic_slice(mat, (first, tp_idx * half), (last - first, half)))
                other.append(lax.dynamic_slice(mat, (first, (1 - tp_idx) * half), (last - first, half)))
            return jnp.concatenate(own, 1), jnp.concatenate(other, 1)

        def column_pieces(mats, rows=None):
            own, other = halves(mats, rows)
            far = over_y(other)
            own_x = over_x(own)
            far_x = over_x(far)
            return [
                own, far, over_core(own), over_core(far),
                own_x, far_x, over_core(own_x), over_core(far_x),
            ]

        def row_pieces(mat):
            aligned = (dp_idx // 2) == tp_idx
            from_x = over_x(mat)
            far = over_y(jnp.where(aligned, from_x, mat))
            near = jnp.where(aligned, mat, from_x)
            return [near, far, over_core(near), over_core(far)]

        def column_slot(piece, me):
            slot = 0
            for bit in (1, 2, 4):
                mine = (me // bit) % 2
                slot = slot + (mine if not piece & bit else 1 - mine) * bit
            return slot

        def row_slot(piece, me):
            core = (me // 2) % 2
            tp = me % 2
            core = core if not piece & 2 else 1 - core
            tp = tp if not piece & 1 else 1 - tp
            return 2 * core + tp

        block = w_head.shape[0]
        model = block * tp_size * dp_size
        kv_half = w_key.shape[2] // 2
        q_half = w_query.shape[2] // 2
        ffn_half = w_gate.shape[2] // 2
        vocab_half = w_head.shape[1] // 2

        o_pieces = row_pieces(w_out[0])
        kvq = column_pieces([w_key[0], w_value[0], w_query[0]])
        k_weight, v_weight, q_weight = place(
            kvq, [((model, kv_half), 0), ((model, kv_half), kv_half), ((model, q_half), 2 * kv_half)], column_slot, block
        )
        gate = column_pieces([w_gate[0]])
        up = column_pieces([w_up[0]])
        (o_weight,) = place(o_pieces, [((q_half, model), 0)], row_slot, block)
        (gate_weight,) = place(gate, [((model, ffn_half), 0)], column_slot, block)
        (up_weight,) = place(up, [((model, ffn_half), 0)], column_slot, block)
        down = row_pieces(w_down[0])
        (down_weight,) = place(down, [((ffn_half, model), 0)], row_slot, w_down.shape[1])

        batch, seq_len, _ = prompts.shape
        kv_count = kv_half // HEAD_DIM
        q_count = q_half // HEAD_DIM
        normed = rms_norm(prompts, norm_attn[0])
        cosines, sines = angles_at(jnp.arange(seq_len))
        keys_raw = jnp.dot(normed, k_weight, preferred_element_type=jnp.float32).reshape(batch, seq_len, kv_count, HEAD_DIM)
        values = jnp.dot(normed, v_weight, preferred_element_type=jnp.float32).astype(jnp.bfloat16).reshape(batch, seq_len, kv_count, HEAD_DIM)
        keys = jnp.transpose(rotate(keys_raw, cosines, sines).astype(jnp.bfloat16), (0, 2, 1, 3))
        values = jnp.transpose(values, (0, 2, 1, 3))

        last = lengths - 1
        hidden = jnp.take_along_axis(prompts, last[:, None, None], axis=1)[:, 0]
        normed_last = rms_norm(hidden, norm_attn[0])
        cos_last, sin_last = angles_at(last)
        queries = jnp.dot(normed_last, q_weight, preferred_element_type=jnp.float32).reshape(batch, q_count, HEAD_DIM)
        queries = rotate(queries, cos_last, sin_last).astype(jnp.bfloat16).reshape(batch, kv_count, q_count // kv_count, HEAD_DIM)
        scores = jnp.einsum("bkgh,bksh->bkgs", queries, keys, preferred_element_type=jnp.float32) * HEAD_DIM ** -0.5
        seen = jnp.arange(seq_len)[None, :]
        key_ok = (seen <= last[:, None]) & (seen < lengths[:, None])
        probs = jax.nn.softmax(jnp.where(key_ok[:, None, None], scores, -1e30), axis=-1).astype(jnp.bfloat16)
        attn = jnp.einsum("bkgs,bksh->bkgh", probs, values, preferred_element_type=jnp.float32)
        attn = attn.astype(jnp.bfloat16).reshape(batch, q_half)

        def add_partials(hidden, partial):
            gathered = lax.all_gather(partial, "tp", axis=0)
            return (hidden.astype(jnp.float32) + jnp.sum(gathered.astype(jnp.float32), axis=0)).astype(jnp.bfloat16)

        hidden = add_partials(hidden, jnp.dot(attn, o_weight, preferred_element_type=jnp.float32).astype(jnp.bfloat16))
        normed_mlp = rms_norm(hidden, norm_mlp[0])
        gate_proj = jnp.dot(normed_mlp, gate_weight, preferred_element_type=jnp.float32)
        up_proj = jnp.dot(normed_mlp, up_weight, preferred_element_type=jnp.float32)
        act = (jax.nn.silu(gate_proj) * up_proj).astype(jnp.bfloat16)
        hidden = add_partials(hidden, jnp.dot(act, down_weight, preferred_element_type=jnp.float32).astype(jnp.bfloat16))
        final = rms_norm(hidden, norm_final)

        per_block = jnp.transpose(final.reshape(batch, -1, block), (1, 0, 2))
        per_block = jnp.pad(per_block, ((0, 0), (0, LOGIT_ROWS - batch), (0, 0)))
        head = None
        acc = jnp.zeros((LOGIT_ROWS, vocab_half), jnp.float32)
        for first, last in zip(HEAD_CUTS, HEAD_CUTS[1:]):
            pieces = column_pieces([w_head], (first, last))
            z = per_block[:, :, first:last]
            head, acc = place_head(pieces, (model, vocab_half), column_slot, block, first, z, acc, head)
        logits = acc[:batch]

        vocab_ids = tp_idx * vocab_half + jnp.arange(vocab_half)
        local_lse = jax.nn.logsumexp(logits, axis=-1)
        local_picked = jnp.sum(jnp.where(vocab_ids[None, :] == targets[:, None], logits, 0.0), axis=-1)
        both = lax.all_gather(jnp.stack([local_lse, local_picked]), "tp", axis=0)
        logprobs = jnp.sum(both[:, 1], axis=0) - jax.nn.logsumexp(both[:, 0], axis=0)
        return (
            q_weight[None], k_weight[None], v_weight[None], o_weight[None], gate_weight[None], up_weight[None], down_weight[None],
            head, keys[None], values[None], logprobs,
        )

    return jax.shard_map(
        layer_program,
        mesh=mesh,
        in_specs=(P("dp", None, None), P("dp"), P("dp"), P(), P(), P(), train_spec, train_spec, train_spec, train_spec, train_spec, train_spec, train_spec, P(("dp", "tp"), None)),
        out_specs=(col_spec, col_spec, col_spec, row_spec, col_spec, col_spec, row_spec, P(None, "tp"), cache_spec, cache_spec, P("dp")),
        check_vma=False,
    )
```

```python
import functools

import jax
import jax.numpy as jnp
from jax import lax
from jax.experimental import pallas as pl
from jax.experimental.pallas import tpu as pltpu
from jax.sharding import PartitionSpec as P


HEAD_DIM = 128
RMS_EPS = 1e-5
ROPE_BASE = 10000.0
SLOTS = 8
LAG = 4
TILE_BYTES = 1 << 20

HEAD_CUTS = (0, 64, 128, 192, 256, 320, 384, 448, 496, 512)
HEAD_TILE = 256
TOKEN_TILE = 256
LOGIT_ROWS = 16


def rms_norm(hidden, gain):
    hidden_f32 = hidden.astype(jnp.float32)
    inv_rms = lax.rsqrt(jnp.mean(hidden_f32 * hidden_f32, axis=-1, keepdims=True) + RMS_EPS)
    return (hidden_f32 * inv_rms * gain.astype(jnp.float32)).astype(jnp.bfloat16)


def angles_at(positions):
    inv_freq = ROPE_BASE ** (-jnp.arange(HEAD_DIM // 2, dtype=jnp.float32) * (2.0 / HEAD_DIM))
    angles = positions.astype(jnp.float32)[..., None, None] * inv_freq
    return jnp.cos(angles), jnp.sin(angles)


def place_kernel(steps, n_in, n_alias, n_out, slot_of, *refs):
    ins = refs[:n_in]
    outs = refs[n_in + n_alias : n_in + n_alias + n_out]
    buf, in_sem, out_sem = refs[n_in + n_alias + n_out :]
    me = lax.axis_index("dp") * 2 + lax.axis_index("tp")

    def load(s):
        piece, row, rows, cols, _ = steps[s]
        slot = s % SLOTS
        return pltpu.make_async_copy(ins[piece].at[pl.ds(row, rows)], buf.at[slot, pl.ds(0, rows), pl.ds(0, cols)], in_sem.at[slot])

    def stores(s):
        piece, row, rows, _, dests = steps[s]
        slot = s % SLOTS
        for out, base, stride, first, width in dests:
            at = base + slot_of(piece, me) * stride + row
            yield pltpu.make_async_copy(
                buf.at[slot, pl.ds(0, rows), pl.ds(first, width)],
                outs[out].at[pl.ds(pl.multiple_of(at, 8), rows)],
                out_sem.at[slot],
            )

    total = len(steps)
    for s in range(total + LAG):
        if s < total:
            if s >= SLOTS:
                for copy in stores(s - SLOTS):
                    copy.wait()
            load(s).start()
        if s >= LAG:
            load(s - LAG).wait()
            for copy in stores(s - LAG):
                copy.start()
    for s in range(max(0, total - SLOTS), total):
        for copy in stores(s):
            copy.wait()


def place(pieces, outputs, slot_of, stride, base=0, into=None):
    rows, cols = pieces[0].shape
    tile = rows
    while tile * cols * 2 > TILE_BYTES and tile % 16 == 0:
        tile //= 2
    steps = []
    for piece in range(len(pieces)):
        for row in range(0, rows, tile):
            dests = [(out, base, stride, first, shape[1]) for out, (shape, first) in enumerate(outputs)]
            steps.append((piece, row, tile, cols, dests))
    alias = [] if into is None else list(into)
    return pl.pallas_call(
        functools.partial(place_kernel, steps, len(pieces), len(alias), len(outputs), slot_of),
        out_shape=[jax.ShapeDtypeStruct(shape, jnp.bfloat16) for shape, _ in outputs],
        in_specs=[pl.BlockSpec(memory_space=pl.ANY)] * (len(pieces) + len(alias)),
        out_specs=[pl.BlockSpec(memory_space=pl.ANY)] * len(outputs),
        scratch_shapes=[
            pltpu.VMEM((SLOTS, tile, cols), jnp.bfloat16),
            pltpu.SemaphoreType.DMA((SLOTS,)),
            pltpu.SemaphoreType.DMA((SLOTS,)),
        ],
        input_output_aliases={len(pieces) + k: k for k in range(len(alias))},
        compiler_params=pltpu.CompilerParams(vmem_limit_bytes=24 << 20),
    )(*pieces, *alias)


def project_kernel(x_ref, gain_ref, w_ref, cos_ref, sin_ref, k_ref, v_ref, q_ref):
    hidden = x_ref[0].astype(jnp.float32)
    inv_rms = lax.rsqrt(jnp.mean(hidden * hidden, axis=-1, keepdims=True) + RMS_EPS)
    normed = (hidden * inv_rms * gain_ref[...].astype(jnp.float32)).astype(jnp.bfloat16)

    def turn(part):
        return part * cos_ref[...] + pltpu.roll(part, HEAD_DIM // 2, 1) * sin_ref[...]

    def four_at(number):
        at = pl.ds(pl.multiple_of(number * 4 * HEAD_DIM, 4 * HEAD_DIM), 4 * HEAD_DIM)
        four = jnp.dot(normed, w_ref[:, at], preferred_element_type=jnp.float32)
        return [four[:, side * HEAD_DIM : (side + 1) * HEAD_DIM] for side in range(4)]

    for side, part in enumerate(four_at(0)):
        k_ref[0, side] = turn(part).astype(jnp.bfloat16)
    for side, part in enumerate(four_at(1)):
        v_ref[0, side] = part.astype(jnp.bfloat16)

    @pl.loop(0, q_ref.shape[1] // 4)
    def _(number):
        for side, part in enumerate(four_at(number + 2)):
            q_ref[0, 4 * number + side] = turn(part).astype(jnp.bfloat16)


def project(prompts, gain, weight, kv_heads, cosines, sines):
    batch, seq_len, model = prompts.shape
    q_heads = weight.shape[1] // HEAD_DIM - 2 * kv_heads
    tile = TOKEN_TILE
    cos_both = jnp.concatenate([cosines, cosines], axis=-1)
    sin_both = jnp.concatenate([-sines, sines], axis=-1)

    def shape(heads):
        return jax.ShapeDtypeStruct((batch, heads, seq_len, HEAD_DIM), jnp.bfloat16)

    def out_spec(heads):
        return pl.BlockSpec((1, heads, tile, HEAD_DIM), lambda b, i: (b, 0, i, 0))

    angle_spec = pl.BlockSpec((tile, HEAD_DIM), lambda b, i: (i, 0))
    counts = (kv_heads, kv_heads, q_heads)
    return pl.pallas_call(
        project_kernel,
        grid=(batch, seq_len // tile),
        out_shape=[shape(heads) for heads in counts],
        in_specs=[
            pl.BlockSpec((1, tile, model), lambda b, i: (b, i, 0)),
            pl.BlockSpec((1, model), lambda b, i: (0, 0)),
            pl.BlockSpec(weight.shape, lambda b, i: (0, 0), pipeline_mode=pl.Buffered(1)),
            angle_spec,
            angle_spec,
        ],
        out_specs=[out_spec(heads) for heads in counts],
        compiler_params=pltpu.CompilerParams(vmem_limit_bytes=60 << 20),
        cost_estimate=pl.CostEstimate(flops=2 * batch * seq_len * model * weight.shape[1], bytes_accessed=2 * prompts.size, transcendentals=0),
        name="project",
    )(prompts, gain, weight, cos_both, sin_both)


def attend_kernel(prompt, length_ref, q_ref, k_ref, v_ref, o_ref):
    block = pl.program_id(1)
    rows = q_ref.shape[2]
    length = length_ref[prompt]
    for count in range(1, k_ref.shape[2] // rows + 1):

        @pl.when(block == count - 1)
        def _(count=count):
            keys = count * rows

            @pl.loop(0, q_ref.shape[1])
            def _(head):
                scores = lax.dot_general(
                    q_ref[0, head], k_ref[0, 0, :keys], (((1,), (1,)), ((), ())), preferred_element_type=jnp.float32
                ) * HEAD_DIM ** -0.5
                query_pos = (count - 1) * rows + lax.broadcasted_iota(jnp.int32, (rows, keys), 0)
                key_pos = lax.broadcasted_iota(jnp.int32, (rows, keys), 1)
                scores = jnp.where((key_pos <= query_pos) & (key_pos < length), scores, -1e30)
                weights = jnp.exp(scores - jnp.max(scores, axis=-1, keepdims=True))
                probs = (weights * (1.0 / jnp.sum(weights, axis=-1, keepdims=True))).astype(jnp.bfloat16)
                out = jnp.dot(probs, v_ref[0, 0, :keys], preferred_element_type=jnp.float32)
                o_ref[:, pl.ds(pl.multiple_of(head * HEAD_DIM, HEAD_DIM), HEAD_DIM)] = out.astype(jnp.bfloat16)


def attend(prompt, lengths, queries, keys, values):
    _, q_heads, seq_len, _ = queries.shape
    kv_heads = keys.shape[1]
    group = q_heads // kv_heads
    tile = TOKEN_TILE
    kv_spec = pl.BlockSpec((1, 1, seq_len, HEAD_DIM), lambda h, i: (prompt, h, 0, 0))
    return pl.pallas_call(
        functools.partial(attend_kernel, prompt),
        grid=(kv_heads, seq_len // tile),
        out_shape=jax.ShapeDtypeStruct((seq_len, q_heads * HEAD_DIM), jnp.bfloat16),
        in_specs=[
            pl.BlockSpec(memory_space=pltpu.SMEM),
            pl.BlockSpec((1, group, tile, HEAD_DIM), lambda h, i: (prompt, h, i, 0)),
            kv_spec,
            kv_spec,
        ],
        out_specs=pl.BlockSpec((tile, group * HEAD_DIM), lambda h, i: (i, h)),
        compiler_params=pltpu.CompilerParams(vmem_limit_bytes=32 << 20),
        cost_estimate=pl.CostEstimate(flops=4 * q_heads * seq_len * seq_len * HEAD_DIM, bytes_accessed=1 << 24, transcendentals=0),
        name="attend",
    )(lengths, queries, keys, values)


def mix_kernel(x_ref, mine_ref, other_ref, gain_ref, hidden_ref, normed_ref):
    total = mine_ref[...].astype(jnp.float32) + other_ref[...].astype(jnp.float32)
    hidden = (x_ref[0].astype(jnp.float32) + total).astype(jnp.bfloat16)
    hidden_ref[...] = hidden
    wide = hidden.astype(jnp.float32)
    inv_rms = lax.rsqrt(jnp.mean(wide * wide, axis=-1, keepdims=True) + RMS_EPS)
    normed_ref[...] = (wide * inv_rms * gain_ref[...].astype(jnp.float32)).astype(jnp.bfloat16)


def mix(prompt, prompts, mine, other, gain):
    rows, model = mine.shape
    tile = 128
    spec = pl.BlockSpec((tile, model), lambda i: (i, 0))
    shape = jax.ShapeDtypeStruct((rows, model), jnp.bfloat16)
    return pl.pallas_call(
        mix_kernel,
        grid=(rows // tile,),
        out_shape=[shape, shape],
        in_specs=[pl.BlockSpec((1, tile, model), lambda i: (prompt, i, 0)), spec, spec, pl.BlockSpec((1, model), lambda i: (0, 0))],
        out_specs=[spec, spec],
        compiler_params=pltpu.CompilerParams(vmem_limit_bytes=32 << 20),
        cost_estimate=pl.CostEstimate(flops=10 * rows * model, bytes_accessed=10 * rows * model, transcendentals=0),
        name="mix",
    )(prompts, mine, other, gain)


def head_kernel(rows, tile, numbers, n_alias, slot_of, *refs):
    n_in = len(numbers)
    z_ref, acc_ref = refs[:2]
    ins = refs[2 : 2 + n_in]
    out_ref, logits_ref, buf, in_sem, out_sem = refs[2 + n_in + n_alias :]
    me = lax.axis_index("dp") * 2 + lax.axis_index("tp")
    base, block, slots, lag = rows
    cols = out_ref.shape[1]
    steps = [(piece, row) for piece in range(n_in) for row in range(0, ins[0].shape[0], tile)]

    def load(s):
        piece, row = steps[s]
        slot = s % slots
        return pltpu.make_async_copy(ins[piece].at[pl.ds(row, tile)], buf.at[slot], in_sem.at[slot])

    def store(s):
        piece, row = steps[s]
        slot = s % slots
        at = pl.multiple_of(slot_of(numbers[piece], me) * block + base + row, 8)
        return pltpu.make_async_copy(buf.at[slot], out_ref.at[pl.ds(at, tile)], out_sem.at[slot])

    logits_ref[...] = acc_ref[...]
    width = cols // 5
    total = len(steps)
    for s in range(total + lag):
        if s < total:
            if s >= slots:
                store(s - slots).wait()
            load(s).start()
        if s >= lag:
            done = s - lag
            piece, row = steps[done]
            load(done).wait()
            store(done).start()
            z = z_ref[slot_of(numbers[piece], me)][:, row : row + tile]

            @pl.loop(0, 5)
            def _(j, z=z, slot=done % slots):
                at = pl.ds(pl.multiple_of(j * width, 128), width)
                logits_ref[:, at] += jnp.dot(z, buf[slot, :, at], preferred_element_type=jnp.float32)

    for s in range(max(0, total - slots), total):
        store(s).wait()


def place_head(numbers, pieces, shape, slot_of, block, base, z, acc, into):
    rows, cols = pieces[0].shape
    tile = min(rows, HEAD_TILE)
    slots, lag = (4, 2) if tile > 128 else (8, 4)
    alias = [] if into is None else [into]
    any_spec = pl.BlockSpec(memory_space=pl.ANY)
    vmem = pl.BlockSpec(memory_space=pltpu.VMEM)
    return pl.pallas_call(
        functools.partial(head_kernel, (base, block, slots, lag), tile, numbers, len(alias), slot_of),
        out_shape=[jax.ShapeDtypeStruct(shape, jnp.bfloat16), jax.ShapeDtypeStruct(acc.shape, jnp.float32)],
        in_specs=[vmem, vmem] + [any_spec] * (len(pieces) + len(alias)),
        out_specs=[any_spec, vmem],
        scratch_shapes=[
            pltpu.VMEM((slots, tile, cols), jnp.bfloat16),
            pltpu.SemaphoreType.DMA((slots,)),
            pltpu.SemaphoreType.DMA((slots,)),
        ],
        input_output_aliases={2 + len(pieces): 0} if alias else {},
        compiler_params=pltpu.CompilerParams(vmem_limit_bytes=48 << 20),
    )(z, acc, *pieces, *alias)


def solution(mesh):
    tp_size = mesh.shape["tp"]
    dp_size = mesh.shape["dp"]
    train_spec = P(None, ("dp", "tp"), None)
    col_spec = P(None, None, "tp")
    row_spec = P(None, "tp", None)
    cache_spec = P(None, "dp", "tp", None, None)
    x_pairs = [(i, i ^ 2) for i in range(dp_size)]
    core_pairs = [(i, i ^ 1) for i in range(dp_size)]
    y_pairs = [(0, 1), (1, 0)]

    def over_x(value):
        return lax.ppermute(value, "dp", x_pairs)

    def over_y(value):
        return lax.ppermute(value, "tp", y_pairs)

    def over_core(value):
        return lax.ppermute(value, "dp", core_pairs)

    def layer_program(prompts, lengths, targets, norm_attn, norm_mlp, norm_final, w_query, w_key, w_value, w_out, w_gate, w_up, w_down, w_head):
        tp_idx = lax.axis_index("tp")
        dp_idx = lax.axis_index("dp")

        def halves(mats, rows=None):
            own, other = [], []
            for mat in mats:
                first, last = (0, mat.shape[0]) if rows is None else rows
                half = mat.shape[1] // 2
                own.append(lax.dynamic_slice(mat, (first, tp_idx * half), (last - first, half)))
                other.append(lax.dynamic_slice(mat, (first, (1 - tp_idx) * half), (last - first, half)))
            return jnp.concatenate(own, 1), jnp.concatenate(other, 1)

        def column_pieces(mats, rows=None):
            own, other = halves(mats, rows)
            far = over_y(other)
            own_x = over_x(own)
            far_x = over_x(far)
            return [
                own, far, over_core(own), over_core(far),
                own_x, far_x, over_core(own_x), over_core(far_x),
            ]

        def row_pieces(mat):
            aligned = (dp_idx // 2) == tp_idx
            from_x = over_x(mat)
            sent = jnp.where(aligned, from_x, mat)
            near = jnp.where(aligned, mat, from_x)
            far = over_y(sent)
            return [near, far, over_core(near), over_core(far)]

        def column_slot(piece, me):
            slot = 0
            for bit in (1, 2, 4):
                mine = (me // bit) % 2
                slot = slot + (mine if not piece & bit else 1 - mine) * bit
            return slot

        def row_slot(piece, me):
            core = (me // 2) % 2
            tp = me % 2
            core = core if not piece & 2 else 1 - core
            tp = tp if not piece & 1 else 1 - tp
            return 2 * core + tp

        block = w_head.shape[0]
        model = block * tp_size * dp_size
        kv_half = w_key.shape[2] // 2
        q_half = w_query.shape[2] // 2
        ffn_half = w_gate.shape[2] // 2
        vocab_half = w_head.shape[1] // 2

        o_pieces = row_pieces(w_out[0])
        kvq = column_pieces([w_key[0], w_value[0], w_query[0]])
        whole_q = 2 * kv_half + q_half
        k_weight, v_weight, q_weight, kvq_weight = place(
            kvq,
            [((model, kv_half), 0), ((model, kv_half), kv_half), ((model, q_half), 2 * kv_half), ((model, whole_q), 0)],
            column_slot, block,
        )
        gate = column_pieces([w_gate[0]])
        up = column_pieces([w_up[0]])
        (o_weight,) = place(o_pieces, [((q_half, model), 0)], row_slot, block)
        (gate_weight,) = place(gate, [((model, ffn_half), 0)], column_slot, block)
        (up_weight,) = place(up, [((model, ffn_half), 0)], column_slot, block)
        down = row_pieces(w_down[0])
        (down_weight,) = place(down, [((ffn_half, model), 0)], row_slot, w_down.shape[1])

        batch, seq_len, _ = prompts.shape
        kv_count = kv_half // HEAD_DIM
        cosines, sines = angles_at(jnp.arange(seq_len))
        keys, values, queries = project(prompts, norm_attn, kvq_weight, kv_count, cosines[:, 0], sines[:, 0])

        hidden, partials = [], []
        for n in range(batch):
            attn = attend(n, lengths, queries, keys, values)
            partial = jnp.dot(attn, o_weight, preferred_element_type=jnp.float32).astype(jnp.bfloat16)
            other = over_y(partial)
            hidden_n, normed_mlp = mix(n, prompts, partial, other, norm_mlp)
            hidden.append(hidden_n)
            gate_proj = jnp.dot(normed_mlp, gate_weight, preferred_element_type=jnp.float32)
            up_proj = jnp.dot(normed_mlp, up_weight, preferred_element_type=jnp.float32)
            act = (jax.nn.silu(gate_proj) * up_proj).astype(jnp.bfloat16)
            partials.append(jnp.dot(act, down_weight, preferred_element_type=jnp.float32).astype(jnp.bfloat16))

        last = lengths - 1

        def last_rows(mats):
            return jnp.concatenate([lax.dynamic_slice_in_dim(mat, last[n], 1, 0) for n, mat in enumerate(mats)], 0)

        partial = last_rows(partials)
        total = partial.astype(jnp.float32) + lax.ppermute(partial, "tp", y_pairs).astype(jnp.float32)
        final = rms_norm((last_rows(hidden).astype(jnp.float32) + total).astype(jnp.bfloat16), norm_final)

        per_block = jnp.transpose(final.reshape(batch, -1, block), (1, 0, 2))
        per_block = jnp.pad(per_block, ((0, 0), (0, LOGIT_ROWS - batch), (0, 0)))
        own, _ = halves([w_head])
        own_x = over_x(own)
        near = {0: own, 2: over_core(own), 4: own_x, 6: over_core(own_x)}
        (head,) = place(
            list(near.values()), [((model, vocab_half), 0)], lambda j, me: column_slot(list(near)[j], me), block
        )
        me = 2 * dp_idx + tp_idx
        acc = sum(jnp.dot(per_block[column_slot(j, me)], piece, preferred_element_type=jnp.float32) for j, piece in near.items())
        for first, last_row in zip(HEAD_CUTS, HEAD_CUTS[1:]):
            _, other = halves([w_head], (first, last_row))
            far = over_y(other)
            far_x = over_x(far)
            pieces = {1: far, 3: over_core(far), 5: far_x, 7: over_core(far_x)}
            head, acc = place_head(
                tuple(pieces), list(pieces.values()), (model, vocab_half), column_slot, block, first, per_block[:, :, first:last_row], acc, head
            )
        logits = acc[:batch]

        vocab_ids = tp_idx * vocab_half + jnp.arange(vocab_half)
        local_lse = jax.nn.logsumexp(logits, axis=-1)
        local_picked = jnp.sum(jnp.where(vocab_ids[None, :] == targets[:, None], logits, 0.0), axis=-1)
        local = jnp.stack([local_lse, local_picked])
        other = lax.ppermute(local, "tp", y_pairs)
        logprobs = local[1] + other[1] - jnp.logaddexp(local[0], other[0])
        return (
            q_weight[None], k_weight[None], v_weight[None], o_weight[None], gate_weight[None], up_weight[None], down_weight[None],
            head, keys[None], values[None], logprobs,
        )

    return jax.shard_map(
        layer_program,
        mesh=mesh,
        in_specs=(P("dp", None, None), P("dp"), P("dp"), P(), P(), P(), train_spec, train_spec, train_spec, train_spec, train_spec, train_spec, train_spec, P(("dp", "tp"), None)),
        out_specs=(col_spec, col_spec, col_spec, row_spec, col_spec, col_spec, row_spec, P(None, "tp"), cache_spec, cache_spec, P("dp")),
        check_vma=False,
    )
```

```python
import functools

import jax
import jax.numpy as jnp
from jax import lax
from jax.experimental import pallas as pl
from jax.experimental.pallas import tpu as pltpu
from jax.sharding import PartitionSpec as P


HEAD_DIM = 128
RMS_EPS = 1e-5
ROPE_BASE = 10000.0
SLOTS = 8
LAG = 4
TILE_BYTES = 1 << 20

HEAD_CUTS = (0, 192, 224, 320, 416, 480, 512)
HEAD_TILE = 96
TOKEN_TILE = 256
PROJECT_TILE = 512
HEADS_AT_ONCE = 2
MASKED = -1e30
EXP2_SCALE = HEAD_DIM ** -0.5 * 1.4426950408889634
LOGIT_ROWS = 16


def rms_norm(hidden, gain):
    hidden_f32 = hidden.astype(jnp.float32)
    inv_rms = lax.rsqrt(jnp.mean(hidden_f32 * hidden_f32, axis=-1, keepdims=True) + RMS_EPS)
    return (hidden_f32 * inv_rms * gain.astype(jnp.float32)).astype(jnp.bfloat16)


def angles_at(positions):
    inv_freq = ROPE_BASE ** (-jnp.arange(HEAD_DIM // 2, dtype=jnp.float32) * (2.0 / HEAD_DIM))
    angles = positions.astype(jnp.float32)[..., None, None] * inv_freq
    return jnp.cos(angles), jnp.sin(angles)


def place_kernel(steps, n_in, n_alias, n_out, slot_of, *refs):
    ins = refs[:n_in]
    outs = refs[n_in + n_alias : n_in + n_alias + n_out]
    buf, in_sem, out_sem = refs[n_in + n_alias + n_out :]
    me = lax.axis_index("dp") * 2 + lax.axis_index("tp")

    def load(s):
        piece, row, rows, cols, _ = steps[s]
        slot = s % SLOTS
        return pltpu.make_async_copy(ins[piece].at[pl.ds(row, rows)], buf.at[slot, pl.ds(0, rows), pl.ds(0, cols)], in_sem.at[slot])

    def stores(s):
        piece, row, rows, _, dests = steps[s]
        slot = s % SLOTS
        for out, base, stride, first, width in dests:
            at = base + slot_of(piece, me) * stride + row
            yield pltpu.make_async_copy(
                buf.at[slot, pl.ds(0, rows), pl.ds(first, width)],
                outs[out].at[pl.ds(pl.multiple_of(at, 8), rows)],
                out_sem.at[slot],
            )

    total = len(steps)
    for s in range(total + LAG):
        if s < total:
            if s >= SLOTS:
                for copy in stores(s - SLOTS):
                    copy.wait()
            load(s).start()
        if s >= LAG:
            load(s - LAG).wait()
            for copy in stores(s - LAG):
                copy.start()
    for s in range(max(0, total - SLOTS), total):
        for copy in stores(s):
            copy.wait()


def place(pieces, outputs, slot_of, stride, base=0, into=None):
    rows, cols = pieces[0].shape
    tile = rows
    while tile * cols * 2 > TILE_BYTES and tile % 16 == 0:
        tile //= 2
    steps = []
    for piece in range(len(pieces)):
        for row in range(0, rows, tile):
            dests = [(out, base, stride, first, shape[1]) for out, (shape, first) in enumerate(outputs)]
            steps.append((piece, row, tile, cols, dests))
    alias = [] if into is None else list(into)
    return pl.pallas_call(
        functools.partial(place_kernel, steps, len(pieces), len(alias), len(outputs), slot_of),
        out_shape=[jax.ShapeDtypeStruct(shape, jnp.bfloat16) for shape, _ in outputs],
        in_specs=[pl.BlockSpec(memory_space=pl.ANY)] * (len(pieces) + len(alias)),
        out_specs=[pl.BlockSpec(memory_space=pl.ANY)] * len(outputs),
        scratch_shapes=[
            pltpu.VMEM((SLOTS, tile, cols), jnp.bfloat16),
            pltpu.SemaphoreType.DMA((SLOTS,)),
            pltpu.SemaphoreType.DMA((SLOTS,)),
        ],
        input_output_aliases={len(pieces) + k: k for k in range(len(alias))},
        compiler_params=pltpu.CompilerParams(vmem_limit_bytes=24 << 20),
    )(*pieces, *alias)


def project_kernel(x_ref, gain_ref, w_ref, cos_ref, sin_ref, k_ref, v_ref, q_ref):
    hidden = x_ref[0].astype(jnp.float32)
    inv_rms = lax.rsqrt(jnp.mean(hidden * hidden, axis=-1, keepdims=True) + RMS_EPS)
    normed = (hidden * inv_rms * gain_ref[...].astype(jnp.float32)).astype(jnp.bfloat16)

    def turn(part):
        return part * cos_ref[...] + pltpu.roll(part, HEAD_DIM // 2, 1) * sin_ref[...]

    def four_at(number):
        at = pl.ds(pl.multiple_of(number * 4 * HEAD_DIM, 4 * HEAD_DIM), 4 * HEAD_DIM)
        four = jnp.dot(normed, w_ref[:, at], preferred_element_type=jnp.float32)
        return [four[:, side * HEAD_DIM : (side + 1) * HEAD_DIM] for side in range(4)]

    for side, part in enumerate(four_at(0)):
        k_ref[0, side] = turn(part).astype(jnp.bfloat16)
    for side, part in enumerate(four_at(1)):
        v_ref[0, side] = part.astype(jnp.bfloat16)

    @pl.loop(0, q_ref.shape[1] // 4)
    def _(number):
        for side, part in enumerate(four_at(number + 2)):
            q_ref[0, 4 * number + side] = turn(part).astype(jnp.bfloat16)


def project(prompts, gain, weight, kv_heads, cosines, sines):
    batch, seq_len, model = prompts.shape
    q_heads = weight.shape[1] // HEAD_DIM - 2 * kv_heads
    tile = PROJECT_TILE
    cos_both = jnp.concatenate([cosines, cosines], axis=-1)
    sin_both = jnp.concatenate([-sines, sines], axis=-1)

    def shape(heads):
        return jax.ShapeDtypeStruct((batch, heads, seq_len, HEAD_DIM), jnp.bfloat16)

    def out_spec(heads):
        return pl.BlockSpec((1, heads, tile, HEAD_DIM), lambda b, i: (b, 0, i, 0))

    angle_spec = pl.BlockSpec((tile, HEAD_DIM), lambda b, i: (i, 0))
    counts = (kv_heads, kv_heads, q_heads)
    return pl.pallas_call(
        project_kernel,
        grid=(batch, seq_len // tile),
        out_shape=[shape(heads) for heads in counts],
        in_specs=[
            pl.BlockSpec((1, tile, model), lambda b, i: (b, i, 0)),
            pl.BlockSpec((1, model), lambda b, i: (0, 0)),
            pl.BlockSpec(weight.shape, lambda b, i: (0, 0), pipeline_mode=pl.Buffered(1)),
            angle_spec,
            angle_spec,
        ],
        out_specs=[out_spec(heads) for heads in counts],
        compiler_params=pltpu.CompilerParams(vmem_limit_bytes=60 << 20),
        cost_estimate=pl.CostEstimate(flops=2 * batch * seq_len * model * weight.shape[1], bytes_accessed=2 * prompts.size, transcendentals=0),
        name="project",
    )(prompts, gain, weight, cos_both, sin_both)


def attend_kernel(prompt, length_ref, q_ref, k_ref, v_ref, o_ref):
    block = pl.program_id(1)
    rows = q_ref.shape[2]
    length = length_ref[prompt]
    contract = (((1,), (1,)), ((), ()))
    for count in range(k_ref.shape[2] // rows):

        @pl.when(block == count)
        def _(count=count):
            first = count * rows
            keys = first + rows
            bias = jnp.where(lax.broadcasted_iota(jnp.int32, (1, keys), 1) < length, 0.0, MASKED)
            causal = lax.broadcasted_iota(jnp.int32, (rows, rows), 1) <= lax.broadcasted_iota(jnp.int32, (rows, rows), 0)

            def one_head(head):
                query = q_ref[0, head]
                near = lax.dot_general(query, k_ref[0, 0, first:keys], contract, preferred_element_type=jnp.float32)
                near = jnp.where(causal, near * EXP2_SCALE + bias[:, first:], MASKED)
                top = jnp.max(near, axis=-1, keepdims=True)
                if count:
                    far = lax.dot_general(query, k_ref[0, 0, :first], contract, preferred_element_type=jnp.float32)
                    far = far * EXP2_SCALE + bias[:, :first]
                    top = jnp.maximum(top, jnp.max(far, axis=-1, keepdims=True))
                    far = jnp.exp2(far - top)
                near = jnp.exp2(near - top)
                total = jnp.sum(near, axis=-1, keepdims=True)
                if count:
                    total += jnp.sum(far, axis=-1, keepdims=True)
                inverse = 1.0 / total
                out = jnp.dot((near * inverse).astype(jnp.bfloat16), v_ref[0, 0, first:keys], preferred_element_type=jnp.float32)
                if count:
                    out += jnp.dot((far * inverse).astype(jnp.bfloat16), v_ref[0, 0, :first], preferred_element_type=jnp.float32)
                o_ref[:, pl.ds(pl.multiple_of(head * HEAD_DIM, HEAD_DIM), HEAD_DIM)] = out.astype(jnp.bfloat16)

            @pl.loop(0, q_ref.shape[1] // HEADS_AT_ONCE)
            def _(step):
                for side in range(HEADS_AT_ONCE):
                    one_head(HEADS_AT_ONCE * step + side)


def attend(prompt, lengths, queries, keys, values):
    _, q_heads, seq_len, _ = queries.shape
    kv_heads = keys.shape[1]
    group = q_heads // kv_heads
    tile = TOKEN_TILE
    kv_spec = pl.BlockSpec((1, 1, seq_len, HEAD_DIM), lambda h, i: (prompt, h, 0, 0))
    return pl.pallas_call(
        functools.partial(attend_kernel, prompt),
        grid=(kv_heads, seq_len // tile),
        out_shape=jax.ShapeDtypeStruct((seq_len, q_heads * HEAD_DIM), jnp.bfloat16),
        in_specs=[
            pl.BlockSpec(memory_space=pltpu.SMEM),
            pl.BlockSpec((1, group, tile, HEAD_DIM), lambda h, i: (prompt, h, i, 0)),
            kv_spec,
            kv_spec,
        ],
        out_specs=pl.BlockSpec((tile, group * HEAD_DIM), lambda h, i: (i, h)),
        compiler_params=pltpu.CompilerParams(vmem_limit_bytes=32 << 20),
        cost_estimate=pl.CostEstimate(flops=4 * q_heads * seq_len * seq_len * HEAD_DIM, bytes_accessed=1 << 24, transcendentals=0),
        name="attend",
    )(lengths, queries, keys, values)


def mix_kernel(x_ref, mine_ref, other_ref, gain_ref, hidden_ref, normed_ref):
    total = mine_ref[...].astype(jnp.float32) + other_ref[...].astype(jnp.float32)
    hidden = (x_ref[0].astype(jnp.float32) + total).astype(jnp.bfloat16)
    hidden_ref[...] = hidden
    wide = hidden.astype(jnp.float32)
    inv_rms = lax.rsqrt(jnp.mean(wide * wide, axis=-1, keepdims=True) + RMS_EPS)
    normed_ref[...] = (wide * inv_rms * gain_ref[...].astype(jnp.float32)).astype(jnp.bfloat16)


def mix(prompt, prompts, mine, other, gain):
    rows, model = mine.shape
    tile = 128
    spec = pl.BlockSpec((tile, model), lambda i: (i, 0))
    shape = jax.ShapeDtypeStruct((rows, model), jnp.bfloat16)
    return pl.pallas_call(
        mix_kernel,
        grid=(rows // tile,),
        out_shape=[shape, shape],
        in_specs=[pl.BlockSpec((1, tile, model), lambda i: (prompt, i, 0)), spec, spec, pl.BlockSpec((1, model), lambda i: (0, 0))],
        out_specs=[spec, spec],
        compiler_params=pltpu.CompilerParams(vmem_limit_bytes=32 << 20),
        cost_estimate=pl.CostEstimate(flops=10 * rows * model, bytes_accessed=10 * rows * model, transcendentals=0),
        name="mix",
    )(prompts, mine, other, gain)


def head_kernel(rows, tile, numbers, n_alias, slot_of, *refs):
    n_in = len(numbers)
    z_ref, acc_ref = refs[:2]
    ins = refs[2 : 2 + n_in]
    out_ref, logits_ref, buf, in_sem, out_sem = refs[2 + n_in + n_alias :]
    me = lax.axis_index("dp") * 2 + lax.axis_index("tp")
    base, block, slots, lag = rows
    cols = out_ref.shape[1]
    steps = [(piece, row) for piece in range(n_in) for row in range(0, ins[0].shape[0], tile)]

    def load(s):
        piece, row = steps[s]
        slot = s % slots
        return pltpu.make_async_copy(ins[piece].at[pl.ds(row, tile)], buf.at[slot], in_sem.at[slot])

    def store(s):
        piece, row = steps[s]
        slot = s % slots
        at = pl.multiple_of(slot_of(numbers[piece], me) * block + base + row, 8)
        return pltpu.make_async_copy(buf.at[slot], out_ref.at[pl.ds(at, tile)], out_sem.at[slot])

    logits_ref[...] = acc_ref[...]
    width = cols // 5
    total = len(steps)
    for s in range(total + lag):
        if s < total:
            if s >= slots:
                store(s - slots).wait()
            load(s).start()
        if s >= lag:
            done = s - lag
            piece, row = steps[done]
            load(done).wait()
            store(done).start()
            z = z_ref[slot_of(numbers[piece], me)][:, row : row + tile]

            @pl.loop(0, 5)
            def _(j, z=z, slot=done % slots):
                at = pl.ds(pl.multiple_of(j * width, 128), width)
                logits_ref[:, at] += jnp.dot(z, buf[slot, :, at], preferred_element_type=jnp.float32)

    for s in range(max(0, total - slots), total):
        store(s).wait()


def near_kernel(numbers, tile, slot_of, z_ref, *refs):
    ins = refs[: len(numbers)]
    logits_ref, buf, sem = refs[len(numbers) :]
    me = lax.axis_index("dp") * 2 + lax.axis_index("tp")
    slots = buf.shape[0]
    cols = buf.shape[2]
    width = cols // 5
    steps = [(piece, row) for piece in range(len(numbers)) for row in range(0, ins[0].shape[0], tile)]

    def load(s):
        piece, row = steps[s]
        return pltpu.make_async_copy(ins[piece].at[pl.ds(row, tile)], buf.at[s % slots], sem.at[s % slots])

    for s in range(slots - 1):
        load(s).start()
    for s, (piece, row) in enumerate(steps):
        if s + slots - 1 < len(steps):
            load(s + slots - 1).start()
        load(s).wait()
        z = z_ref[slot_of(numbers[piece], me)][:, row : row + tile]

        @pl.loop(0, 5)
        def _(j, z=z, s=s):
            at = pl.ds(pl.multiple_of(j * width, 128), width)
            part = jnp.dot(z, buf[s % slots, :, at], preferred_element_type=jnp.float32)
            logits_ref[:, at] = part if s == 0 else logits_ref[:, at] + part


def near_logits(numbers, pieces, slot_of, z):
    _, cols = pieces[0].shape
    tile, slots = 256, 5
    vmem = pl.BlockSpec(memory_space=pltpu.VMEM)
    return pl.pallas_call(
        functools.partial(near_kernel, numbers, tile, slot_of),
        out_shape=jax.ShapeDtypeStruct((LOGIT_ROWS, cols), jnp.float32),
        in_specs=[vmem] + [pl.BlockSpec(memory_space=pl.ANY)] * len(pieces),
        out_specs=vmem,
        scratch_shapes=[pltpu.VMEM((slots, tile, cols), jnp.bfloat16), pltpu.SemaphoreType.DMA((slots,))],
        compiler_params=pltpu.CompilerParams(vmem_limit_bytes=52 << 20),
        name="near_logits",
    )(z, *pieces)


def place_head(numbers, pieces, shape, slot_of, block, base, z, acc, into):
    rows, cols = pieces[0].shape
    tile = min(rows, HEAD_TILE)
    slots, lag = (4, 2) if tile > 128 else (8, 4)
    alias = [] if into is None else [into]
    any_spec = pl.BlockSpec(memory_space=pl.ANY)
    vmem = pl.BlockSpec(memory_space=pltpu.VMEM)
    return pl.pallas_call(
        functools.partial(head_kernel, (base, block, slots, lag), tile, numbers, len(alias), slot_of),
        out_shape=[jax.ShapeDtypeStruct(shape, jnp.bfloat16), jax.ShapeDtypeStruct(acc.shape, jnp.float32)],
        in_specs=[vmem, vmem] + [any_spec] * (len(pieces) + len(alias)),
        out_specs=[any_spec, vmem],
        scratch_shapes=[
            pltpu.VMEM((slots, tile, cols), jnp.bfloat16),
            pltpu.SemaphoreType.DMA((slots,)),
            pltpu.SemaphoreType.DMA((slots,)),
        ],
        input_output_aliases={2 + len(pieces): 0} if alias else {},
        compiler_params=pltpu.CompilerParams(vmem_limit_bytes=48 << 20),
    )(z, acc, *pieces, *alias)


def solution(mesh):
    tp_size = mesh.shape["tp"]
    dp_size = mesh.shape["dp"]
    train_spec = P(None, ("dp", "tp"), None)
    col_spec = P(None, None, "tp")
    row_spec = P(None, "tp", None)
    cache_spec = P(None, "dp", "tp", None, None)
    x_pairs = [(i, i ^ 2) for i in range(dp_size)]
    core_pairs = [(i, i ^ 1) for i in range(dp_size)]
    y_pairs = [(0, 1), (1, 0)]

    def over_x(value):
        return lax.ppermute(value, "dp", x_pairs)

    def over_y(value):
        return lax.ppermute(value, "tp", y_pairs)

    def over_core(value):
        return lax.ppermute(value, "dp", core_pairs)

    def layer_program(prompts, lengths, targets, norm_attn, norm_mlp, norm_final, w_query, w_key, w_value, w_out, w_gate, w_up, w_down, w_head):
        tp_idx = lax.axis_index("tp")
        dp_idx = lax.axis_index("dp")

        def halves(mats, rows=None):
            own, other = [], []
            for mat in mats:
                first, last = (0, mat.shape[0]) if rows is None else rows
                half = mat.shape[1] // 2
                own.append(lax.dynamic_slice(mat, (first, tp_idx * half), (last - first, half)))
                other.append(lax.dynamic_slice(mat, (first, (1 - tp_idx) * half), (last - first, half)))
            return jnp.concatenate(own, 1), jnp.concatenate(other, 1)

        def column_pieces(mats, rows=None):
            own, other = halves(mats, rows)
            far = over_y(other)
            own_x = over_x(own)
            far_x = over_x(far)
            return [
                own, far, over_core(own), over_core(far),
                own_x, far_x, over_core(own_x), over_core(far_x),
            ]

        def row_pieces(mat):
            aligned = (dp_idx // 2) == tp_idx
            from_x = over_x(mat)
            sent = jnp.where(aligned, from_x, mat)
            near = jnp.where(aligned, mat, from_x)
            far = over_y(sent)
            return [near, far, over_core(near), over_core(far)]

        def column_slot(piece, me):
            slot = 0
            for bit in (1, 2, 4):
                mine = (me // bit) % 2
                slot = slot + (mine if not piece & bit else 1 - mine) * bit
            return slot

        def row_slot(piece, me):
            core = (me // 2) % 2
            tp = me % 2
            core = core if not piece & 2 else 1 - core
            tp = tp if not piece & 1 else 1 - tp
            return 2 * core + tp

        block = w_head.shape[0]
        model = block * tp_size * dp_size
        kv_half = w_key.shape[2] // 2
        q_half = w_query.shape[2] // 2
        ffn_half = w_gate.shape[2] // 2
        vocab_half = w_head.shape[1] // 2

        o_pieces = row_pieces(w_out[0])
        kvq = column_pieces([w_key[0], w_value[0], w_query[0]])
        whole_q = 2 * kv_half + q_half
        k_weight, v_weight, q_weight, kvq_weight = place(
            kvq,
            [((model, kv_half), 0), ((model, kv_half), kv_half), ((model, q_half), 2 * kv_half), ((model, whole_q), 0)],
            column_slot, block,
        )
        gate = column_pieces([w_gate[0]])
        up = column_pieces([w_up[0]])
        (o_weight,) = place(o_pieces, [((q_half, model), 0)], row_slot, block)
        (gate_weight,) = place(gate, [((model, ffn_half), 0)], column_slot, block)
        (up_weight,) = place([up[j] for j in (0, 2, 4, 6)], [((model, ffn_half), 0)], lambda j, me: column_slot(2 * j, me), block)
        (up_weight,) = place(
            [up[j] for j in (1, 3, 5, 7)], [((model, ffn_half), 0)], lambda j, me: column_slot(2 * j + 1, me), block, into=[up_weight]
        )
        rows = w_down.shape[1]
        down_weight = None
        for n, (first, end) in enumerate(((0, 4 * rows // 7), (4 * rows // 7, rows))):
            half = lax.slice_in_dim(w_down[0], first, end, axis=0)
            pieces = row_pieces(half)
            (down_weight,) = place(
                pieces, [((ffn_half, model), 0)], row_slot, rows, base=first, into=None if n == 0 else [down_weight]
            )

        batch, seq_len, _ = prompts.shape
        kv_count = kv_half // HEAD_DIM
        cosines, sines = angles_at(jnp.arange(seq_len))
        keys, values, queries = project(prompts, norm_attn, kvq_weight, kv_count, cosines[:, 0], sines[:, 0])

        hidden, partials = [], []
        for n in range(batch):
            attn = attend(n, lengths, queries, keys, values)
            partial = jnp.dot(attn, o_weight, preferred_element_type=jnp.float32).astype(jnp.bfloat16)
            other = over_y(partial)
            hidden_n, normed_mlp = mix(n, prompts, partial, other, norm_mlp)
            hidden.append(hidden_n)
            gate_proj = jnp.dot(normed_mlp, gate_weight, preferred_element_type=jnp.float32)
            up_proj = jnp.dot(normed_mlp, up_weight, preferred_element_type=jnp.float32)
            act = (jax.nn.silu(gate_proj) * up_proj).astype(jnp.bfloat16)
            partials.append(jnp.dot(act, down_weight, preferred_element_type=jnp.float32).astype(jnp.bfloat16))

        last = lengths - 1

        def last_rows(mats):
            return jnp.concatenate([lax.dynamic_slice_in_dim(mat, last[n], 1, 0) for n, mat in enumerate(mats)], 0)

        partial = last_rows(partials)
        total = partial.astype(jnp.float32) + lax.ppermute(partial, "tp", y_pairs).astype(jnp.float32)
        final = rms_norm((last_rows(hidden).astype(jnp.float32) + total).astype(jnp.bfloat16), norm_final)

        per_block = jnp.transpose(final.reshape(batch, -1, block), (1, 0, 2))
        per_block = jnp.pad(per_block, ((0, 0), (0, LOGIT_ROWS - batch), (0, 0)))
        own, _ = halves([w_head])
        own_x = over_x(own)
        near = {0: own, 2: over_core(own), 4: own_x, 6: over_core(own_x)}
        (head,) = place([near[0], near[2]], [((model, vocab_half), 0)], lambda j, me: column_slot((0, 2)[j], me), block)
        (head,) = place(
            [near[4], near[6]], [((model, vocab_half), 0)], lambda j, me: column_slot((4, 6)[j], me), block, into=[head]
        )
        acc = near_logits(tuple(near), list(near.values()), column_slot, per_block)
        for first, last_row in zip(HEAD_CUTS, HEAD_CUTS[1:]):
            _, other = halves([w_head], (first, last_row))
            far = over_y(other)
            far_x = over_x(far)
            pieces = {1: far, 3: over_core(far), 5: far_x, 7: over_core(far_x)}
            head, acc = place_head(
                tuple(pieces), list(pieces.values()), (model, vocab_half), column_slot, block, first, per_block[:, :, first:last_row], acc, head
            )
        logits = acc[:batch]

        vocab_ids = tp_idx * vocab_half + jnp.arange(vocab_half)
        local_lse = jax.nn.logsumexp(logits, axis=-1)
        local_picked = jnp.sum(jnp.where(vocab_ids[None, :] == targets[:, None], logits, 0.0), axis=-1)
        local = jnp.stack([local_lse, local_picked])
        other = lax.ppermute(local, "tp", y_pairs)
        logprobs = local[1] + other[1] - jnp.logaddexp(local[0], other[0])
        return (
            q_weight[None], k_weight[None], v_weight[None], o_weight[None], gate_weight[None], up_weight[None], down_weight[None],
            head, keys[None], values[None], logprobs,
        )

    return jax.shard_map(
        layer_program,
        mesh=mesh,
        in_specs=(P("dp", None, None), P("dp"), P("dp"), P(), P(), P(), train_spec, train_spec, train_spec, train_spec, train_spec, train_spec, train_spec, P(("dp", "tp"), None)),
        out_specs=(col_spec, col_spec, col_spec, row_spec, col_spec, col_spec, row_spec, P(None, "tp"), cache_spec, cache_spec, P("dp")),
        check_vma=False,
    )
```

```python
import functools

import jax
import jax.numpy as jnp
from jax import lax
from jax.experimental import pallas as pl
from jax.experimental.pallas import tpu as pltpu
from jax.sharding import PartitionSpec as P


HEAD_DIM = 128
RMS_EPS = 1e-5
ROPE_BASE = 10000.0
SLOTS = 8
LAG = 4
TILE_BYTES = 1 << 20

HEAD_CUTS = (0, 256, 384, 512)
QUERY_CUTS = (0, 352, 448, 512)
HEAD_TILE = 256
TOKEN_TILE = 256
LOGIT_ROWS = 16


def rms_norm(hidden, gain):
    hidden_f32 = hidden.astype(jnp.float32)
    inv_rms = lax.rsqrt(jnp.mean(hidden_f32 * hidden_f32, axis=-1, keepdims=True) + RMS_EPS)
    return (hidden_f32 * inv_rms * gain.astype(jnp.float32)).astype(jnp.bfloat16)


def rotate(projected, cosines, sines):
    half_dim = HEAD_DIM // 2
    first_half = projected[..., :half_dim]
    second_half = projected[..., half_dim:]
    return jnp.concatenate([first_half * cosines - second_half * sines, second_half * cosines + first_half * sines], axis=-1)


def angles_at(positions):
    inv_freq = ROPE_BASE ** (-jnp.arange(HEAD_DIM // 2, dtype=jnp.float32) * (2.0 / HEAD_DIM))
    angles = positions.astype(jnp.float32)[..., None, None] * inv_freq
    return jnp.cos(angles), jnp.sin(angles)


def place_kernel(steps, n_in, n_alias, n_out, slot_of, *refs):
    ins = refs[:n_in]
    outs = refs[n_in + n_alias : n_in + n_alias + n_out]
    buf, in_sem, out_sem = refs[n_in + n_alias + n_out :]
    me = lax.axis_index("dp") * 2 + lax.axis_index("tp")

    def load(s):
        piece, row, rows, cols, _ = steps[s]
        slot = s % SLOTS
        return pltpu.make_async_copy(ins[piece].at[pl.ds(row, rows)], buf.at[slot, pl.ds(0, rows), pl.ds(0, cols)], in_sem.at[slot])

    def stores(s):
        piece, row, rows, _, dests = steps[s]
        slot = s % SLOTS
        for out, base, stride, first, width in dests:
            at = base + slot_of(piece, me) * stride + row
            yield pltpu.make_async_copy(
                buf.at[slot, pl.ds(0, rows), pl.ds(first, width)],
                outs[out].at[pl.ds(pl.multiple_of(at, 8), rows)],
                out_sem.at[slot],
            )

    total = len(steps)
    for s in range(total + LAG):
        if s < total:
            if s >= SLOTS:
                for copy in stores(s - SLOTS):
                    copy.wait()
            load(s).start()
        if s >= LAG:
            load(s - LAG).wait()
            for copy in stores(s - LAG):
                copy.start()
    for s in range(max(0, total - SLOTS), total):
        for copy in stores(s):
            copy.wait()


def place(pieces, outputs, slot_of, stride, base=0, into=None):
    rows, cols = pieces[0].shape
    tile = rows
    while tile * cols * 2 > TILE_BYTES and tile % 16 == 0:
        tile //= 2
    steps = []
    for piece in range(len(pieces)):
        for row in range(0, rows, tile):
            dests = [(out, base, stride, first, shape[1]) for out, (shape, first) in enumerate(outputs)]
            steps.append((piece, row, tile, cols, dests))
    alias = [] if into is None else list(into)
    return pl.pallas_call(
        functools.partial(place_kernel, steps, len(pieces), len(alias), len(outputs), slot_of),
        out_shape=[jax.ShapeDtypeStruct(shape, jnp.bfloat16) for shape, _ in outputs],
        in_specs=[pl.BlockSpec(memory_space=pl.ANY)] * (len(pieces) + len(alias)),
        out_specs=[pl.BlockSpec(memory_space=pl.ANY)] * len(outputs),
        scratch_shapes=[
            pltpu.VMEM((SLOTS, tile, cols), jnp.bfloat16),
            pltpu.SemaphoreType.DMA((SLOTS,)),
            pltpu.SemaphoreType.DMA((SLOTS,)),
        ],
        input_output_aliases={len(pieces) + k: k for k in range(len(alias))},
        compiler_params=pltpu.CompilerParams(vmem_limit_bytes=24 << 20),
    )(*pieces, *alias)


def project_kernel(x_ref, gain_ref, w_ref, cos_ref, sin_ref, k_ref, v_ref):
    hidden = x_ref[0].astype(jnp.float32)
    inv_rms = lax.rsqrt(jnp.mean(hidden * hidden, axis=-1, keepdims=True) + RMS_EPS)
    normed = (hidden * inv_rms * gain_ref[...].astype(jnp.float32)).astype(jnp.bfloat16)
    heads = k_ref.shape[1]
    for head in range(2 * heads):
        cols = pl.ds(head * HEAD_DIM, HEAD_DIM)
        if head % 2 == 0:
            pair = jnp.dot(normed, w_ref[:, pl.ds(head * HEAD_DIM, 2 * HEAD_DIM)], preferred_element_type=jnp.float32)
        part = pair[:, (head % 2) * HEAD_DIM : (head % 2 + 1) * HEAD_DIM]
        if head < heads:
            turned = part * cos_ref[...] + pltpu.roll(part, HEAD_DIM // 2, 1) * sin_ref[...]
            k_ref[0, head] = turned.astype(jnp.bfloat16)
        else:
            v_ref[0, head - heads] = part.astype(jnp.bfloat16)


def project(prompts, gain, weight, cosines, sines):
    batch, seq_len, model = prompts.shape
    heads = weight.shape[1] // (2 * HEAD_DIM)
    tile = TOKEN_TILE
    cos_both = jnp.concatenate([cosines, cosines], axis=-1)
    sin_both = jnp.concatenate([-sines, sines], axis=-1)
    shape = jax.ShapeDtypeStruct((batch, heads, seq_len, HEAD_DIM), jnp.bfloat16)
    out_spec = pl.BlockSpec((1, heads, tile, HEAD_DIM), lambda b, i: (b, 0, i, 0))
    angle_spec = pl.BlockSpec((tile, HEAD_DIM), lambda b, i: (i, 0))
    return pl.pallas_call(
        project_kernel,
        grid=(batch, seq_len // tile),
        out_shape=[shape, shape],
        in_specs=[
            pl.BlockSpec((1, tile, model), lambda b, i: (b, i, 0)),
            pl.BlockSpec((1, model), lambda b, i: (0, 0)),
            pl.BlockSpec(weight.shape, lambda b, i: (0, 0)),
            angle_spec,
            angle_spec,
        ],
        out_specs=[out_spec, out_spec],
        compiler_params=pltpu.CompilerParams(vmem_limit_bytes=56 << 20),
        cost_estimate=pl.CostEstimate(flops=2 * batch * seq_len * model * weight.shape[1], bytes_accessed=2 * prompts.size, transcendentals=0),
        name="project",
    )(prompts, gain, weight, cos_both, sin_both)


def head_kernel(rows, tile, numbers, n_alias, slot_of, *refs):
    n_in = len(numbers)
    z_ref, acc_ref = refs[:2]
    ins = refs[2 : 2 + n_in]
    out_ref, logits_ref, buf, in_sem, out_sem = refs[2 + n_in + n_alias :]
    me = lax.axis_index("dp") * 2 + lax.axis_index("tp")
    base, block, slots, lag = rows
    cols = out_ref.shape[1]
    steps = [(piece, row) for piece in range(n_in) for row in range(0, ins[0].shape[0], tile)]

    def load(s):
        piece, row = steps[s]
        slot = s % slots
        return pltpu.make_async_copy(ins[piece].at[pl.ds(row, tile)], buf.at[slot], in_sem.at[slot])

    def store(s):
        piece, row = steps[s]
        slot = s % slots
        at = pl.multiple_of(slot_of(numbers[piece], me) * block + base + row, 8)
        return pltpu.make_async_copy(buf.at[slot], out_ref.at[pl.ds(at, tile)], out_sem.at[slot])

    logits_ref[...] = acc_ref[...]
    width = cols // 5
    total = len(steps)
    for s in range(total + lag):
        if s < total:
            if s >= slots:
                store(s - slots).wait()
            load(s).start()
        if s >= lag:
            done = s - lag
            piece, row = steps[done]
            load(done).wait()
            store(done).start()
            z = z_ref[slot_of(numbers[piece], me)][:, row : row + tile]

            @pl.loop(0, 5)
            def _(j, z=z, slot=done % slots):
                at = pl.ds(pl.multiple_of(j * width, 128), width)
                logits_ref[:, at] += jnp.dot(z, buf[slot, :, at], preferred_element_type=jnp.float32)

    for s in range(max(0, total - slots), total):
        store(s).wait()


def finish_kernel(numbers, slot_of, z_ref, acc_ref, target_ref, *refs):
    ins = refs[: len(numbers)]
    out_ref = refs[len(numbers)]
    me = lax.axis_index("dp") * 2 + lax.axis_index("tp")
    logits = acc_ref[...]
    for number, piece in zip(numbers, ins):
        logits += jnp.dot(z_ref[slot_of(number, me)], piece[...], preferred_element_type=jnp.float32)
    ids = lax.broadcasted_iota(jnp.int32, logits.shape, 1) + lax.axis_index("tp") * logits.shape[1]
    top = jnp.max(logits, axis=-1, keepdims=True)
    lse = top + jnp.log(jnp.sum(jnp.exp(logits - top), axis=-1, keepdims=True))
    picked = jnp.sum(jnp.where(ids == target_ref[...], logits, 0.0), axis=-1, keepdims=True)
    lane = lax.broadcasted_iota(jnp.int32, out_ref.shape, 1)
    out_ref[...] = jnp.where(lane == 0, lse, picked)


def finish(numbers, pieces, slot_of, z, acc, targets):
    vmem = pl.BlockSpec(memory_space=pltpu.VMEM)
    return pl.pallas_call(
        functools.partial(finish_kernel, numbers, slot_of),
        out_shape=jax.ShapeDtypeStruct((acc.shape[0], HEAD_DIM), jnp.float32),
        in_specs=[vmem] * (3 + len(pieces)),
        out_specs=vmem,
        compiler_params=pltpu.CompilerParams(vmem_limit_bytes=32 << 20),
        name="finish",
    )(z, acc, targets, *pieces)


def place_head(numbers, pieces, shape, slot_of, block, base, z, acc, into):
    rows, cols = pieces[0].shape
    tile = min(rows, HEAD_TILE)
    slots, lag = (4, 2) if tile > 128 else (8, 4)
    alias = [] if into is None else [into]
    any_spec = pl.BlockSpec(memory_space=pl.ANY)
    vmem = pl.BlockSpec(memory_space=pltpu.VMEM)
    return pl.pallas_call(
        functools.partial(head_kernel, (base, block, slots, lag), tile, numbers, len(alias), slot_of),
        out_shape=[jax.ShapeDtypeStruct(shape, jnp.bfloat16), jax.ShapeDtypeStruct(acc.shape, jnp.float32)],
        in_specs=[vmem, vmem] + [any_spec] * (len(pieces) + len(alias)),
        out_specs=[any_spec, vmem],
        scratch_shapes=[
            pltpu.VMEM((slots, tile, cols), jnp.bfloat16),
            pltpu.SemaphoreType.DMA((slots,)),
            pltpu.SemaphoreType.DMA((slots,)),
        ],
        input_output_aliases={2 + len(pieces): 0} if alias else {},
        compiler_params=pltpu.CompilerParams(vmem_limit_bytes=48 << 20),
    )(z, acc, *pieces, *alias)


def solution(mesh):
    tp_size = mesh.shape["tp"]
    dp_size = mesh.shape["dp"]
    train_spec = P(None, ("dp", "tp"), None)
    col_spec = P(None, None, "tp")
    row_spec = P(None, "tp", None)
    cache_spec = P(None, "dp", "tp", None, None)
    x_pairs = [(i, i ^ 2) for i in range(dp_size)]
    core_pairs = [(i, i ^ 1) for i in range(dp_size)]
    y_pairs = [(0, 1), (1, 0)]

    def over_x(value):
        return lax.ppermute(value, "dp", x_pairs)

    def over_y(value):
        return lax.ppermute(value, "tp", y_pairs)

    def over_core(value):
        return lax.ppermute(value, "dp", core_pairs)

    def layer_program(prompts, lengths, targets, norm_attn, norm_mlp, norm_final, w_query, w_key, w_value, w_out, w_gate, w_up, w_down, w_head):
        tp_idx = lax.axis_index("tp")
        dp_idx = lax.axis_index("dp")

        def halves(mats, rows=None):
            own, other = [], []
            for mat in mats:
                first, last = (0, mat.shape[0]) if rows is None else rows
                half = mat.shape[1] // 2
                own.append(lax.dynamic_slice(mat, (first, tp_idx * half), (last - first, half)))
                other.append(lax.dynamic_slice(mat, (first, (1 - tp_idx) * half), (last - first, half)))
            return jnp.concatenate(own, 1), jnp.concatenate(other, 1)

        def column_pieces(mats, rows=None):
            own, other = halves(mats, rows)
            far = over_y(other)
            own_x = over_x(own)
            far_x = over_x(far)
            return [
                own, far, over_core(own), over_core(far),
                own_x, far_x, over_core(own_x), over_core(far_x),
            ]

        def row_pieces(mat):
            aligned = (dp_idx // 2) == tp_idx
            from_x = over_x(mat)
            far = over_y(jnp.where(aligned, from_x, mat))
            near = jnp.where(aligned, mat, from_x)
            return [near, far, over_core(near), over_core(far)]

        def column_slot(piece, me):
            slot = 0
            for bit in (1, 2, 4):
                mine = (me // bit) % 2
                slot = slot + (mine if not piece & bit else 1 - mine) * bit
            return slot

        def row_slot(piece, me):
            core = (me // 2) % 2
            tp = me % 2
            core = core if not piece & 2 else 1 - core
            tp = tp if not piece & 1 else 1 - tp
            return 2 * core + tp

        block = w_head.shape[0]
        model = block * tp_size * dp_size
        kv_half = w_key.shape[2] // 2
        q_half = w_query.shape[2] // 2
        ffn_half = w_gate.shape[2] // 2
        vocab_half = w_head.shape[1] // 2

        o_pieces = row_pieces(w_out[0])
        kvq = column_pieces([w_key[0], w_value[0]])
        k_weight, v_weight, kv_weight = place(
            kvq, [((model, kv_half), 0), ((model, kv_half), kv_half), ((model, 2 * kv_half), 0)], column_slot, block
        )
        gate = column_pieces([w_gate[0]])
        up = column_pieces([w_up[0]])
        (o_weight,) = place(o_pieces, [((q_half, model), 0)], row_slot, block)
        (gate_weight,) = place(gate, [((model, ffn_half), 0)], column_slot, block)
        (up_weight,) = place(up, [((model, ffn_half), 0)], column_slot, block)
        down = row_pieces(w_down[0])
        (down_weight,) = place(down, [((ffn_half, model), 0)], row_slot, w_down.shape[1])

        batch, seq_len, _ = prompts.shape
        kv_count = kv_half // HEAD_DIM
        q_count = q_half // HEAD_DIM
        cosines, sines = angles_at(jnp.arange(seq_len))
        keys, values = project(prompts, norm_attn, kv_weight, cosines[:, 0], sines[:, 0])

        last = lengths - 1
        hidden = jnp.take_along_axis(prompts, last[:, None, None], axis=1)[:, 0]
        normed_last = rms_norm(hidden, norm_attn[0])
        cos_last, sin_last = angles_at(last)

        core_idx = dp_idx % 2
        me = 2 * dp_idx + tp_idx
        sibling = over_core(normed_last)
        pair = jnp.concatenate([jnp.where(core_idx == 0, normed_last, sibling), jnp.where(core_idx == 0, sibling, normed_last)], 0)
        far_rows = over_x(lax.dynamic_slice_in_dim(pair, column_slot(4, me) * block, block, 1))
        both = jnp.concatenate([lax.dynamic_slice_in_dim(pair, me * block, block, 1), far_rows], 0)
        part = jnp.dot(both, w_query[0], preferred_element_type=jnp.float32)
        own_part = lax.dynamic_slice_in_dim(part, tp_idx * q_half, q_half, 1)
        other_part = lax.dynamic_slice_in_dim(part, (1 - tp_idx) * q_half, q_half, 1)
        part = own_part + over_y(other_part)
        part = part + over_core(part)
        near_part = lax.dynamic_slice_in_dim(part, core_idx * batch, batch, 0)
        far_part = lax.dynamic_slice_in_dim(part, 2 * batch + core_idx * batch, batch, 0)
        queries = (near_part + over_x(far_part)).reshape(batch, q_count, HEAD_DIM)
        queries = rotate(queries, cos_last, sin_last).astype(jnp.bfloat16).reshape(batch, kv_count, q_count // kv_count, HEAD_DIM)
        scores = jnp.einsum("bkgh,bksh->bkgs", queries, keys, preferred_element_type=jnp.float32) * HEAD_DIM ** -0.5
        seen = jnp.arange(seq_len)[None, :]
        key_ok = (seen <= last[:, None]) & (seen < lengths[:, None])
        probs = jax.nn.softmax(jnp.where(key_ok[:, None, None], scores, -1e30), axis=-1).astype(jnp.bfloat16)
        attn = jnp.einsum("bkgs,bksh->bkgh", probs, values, preferred_element_type=jnp.float32)
        attn = attn.astype(jnp.bfloat16).reshape(batch, q_half)

        def add_partials(hidden, partial):
            total = partial.astype(jnp.float32) + lax.ppermute(partial, "tp", y_pairs).astype(jnp.float32)
            return (hidden.astype(jnp.float32) + total).astype(jnp.bfloat16)

        hidden = add_partials(hidden, jnp.dot(attn, o_weight, preferred_element_type=jnp.float32).astype(jnp.bfloat16))
        normed_mlp = rms_norm(hidden, norm_mlp[0])
        gate_proj = jnp.dot(normed_mlp, gate_weight, preferred_element_type=jnp.float32)
        up_proj = jnp.dot(normed_mlp, up_weight, preferred_element_type=jnp.float32)
        act = (jax.nn.silu(gate_proj) * up_proj).astype(jnp.bfloat16)
        hidden = add_partials(hidden, jnp.dot(act, down_weight, preferred_element_type=jnp.float32).astype(jnp.bfloat16))
        final = rms_norm(hidden, norm_final)

        per_block = jnp.transpose(final.reshape(batch, -1, block), (1, 0, 2))
        per_block = jnp.pad(per_block, ((0, 0), (0, LOGIT_ROWS - batch), (0, 0)))
        head = None
        acc = jnp.zeros((LOGIT_ROWS, vocab_half), jnp.float32)
        for first, last in zip(HEAD_CUTS, HEAD_CUTS[1:]):
            pieces = column_pieces([w_head], (first, last))
            z = per_block[:, :, first:last]
            head, acc = place_head(tuple(range(8)), pieces, (model, vocab_half), column_slot, block, first, z, acc, head)
        target_rows = jnp.pad(targets, (0, LOGIT_ROWS - batch))[:, None]
        mine = finish((), [], column_slot, z, acc, target_rows)
        other = over_y(mine)
        logprobs = (mine[:, 1] + other[:, 1] - jnp.logaddexp(mine[:, 0], other[:, 0]))[:batch]

        own, other = halves([w_query[0]])
        far = over_y(other)
        own_x = over_x(own)
        early = {0: own, 1: far, 2: over_core(own), 3: over_core(far), 4: own_x, 6: over_core(own_x)}
        numbers = tuple(early)
        (q_weight,) = place(
            list(early.values()), [((model, q_half), 0)], lambda j, me: column_slot(numbers[j], me), block
        )
        for first, end in zip(QUERY_CUTS, QUERY_CUTS[1:]):
            far_x = over_x(lax.slice_in_dim(far, first, end, axis=0))
            rest = [far_x, over_core(far_x)]
            (q_weight,) = place(
                rest, [((model, q_half), 0)], lambda j, me: column_slot((5, 7)[j], me), block, base=first, into=[q_weight]
            )
        return (
            q_weight[None], k_weight[None], v_weight[None], o_weight[None], gate_weight[None], up_weight[None], down_weight[None],
            head, keys[None], values[None], logprobs,
        )

    return jax.shard_map(
        layer_program,
        mesh=mesh,
        in_specs=(P("dp", None, None), P("dp"), P("dp"), P(), P(), P(), train_spec, train_spec, train_spec, train_spec, train_spec, train_spec, train_spec, P(("dp", "tp"), None)),
        out_specs=(col_spec, col_spec, col_spec, row_spec, col_spec, col_spec, row_spec, P(None, "tp"), cache_spec, cache_spec, P("dp")),
        check_vma=False,
    )
```
